32 devices in a mesh: rows: 4 (over z), model: 8 (over y, x, core).
Axes of the slice: x: 2, y: 2, z: 4, core: 2. Of those that a mesh axis runs over, the one named last changes fastest.
Arguments:
- train_query: bfloat16 [8192, 8192], P('rows', 'model'), may hold values from -0.0625 to 0.0625
- low_query: bfloat16 [8192, 16], P('rows'), may hold values from -0.0625 to 0.0625
- high_query: bfloat16 [16, 8192], P(None, 'model'), may hold values from -1.5 to 1.5
- train_key: bfloat16 [8192, 1024], P('rows', 'model'), may hold values from -0.0625 to 0.0625
- low_key: bfloat16 [8192, 16], P('rows'), may hold values from -0.0625 to 0.0625
- high_key: bfloat16 [16, 1024], P(None, 'model'), may hold values from -1.5 to 1.5
- train_value: bfloat16 [8192, 1024], P('rows', 'model'), may hold values from -0.0625 to 0.0625
- low_value: bfloat16 [8192, 16], P('rows'), may hold values from -0.0625 to 0.0625
- high_value: bfloat16 [16, 1024], P(None, 'model'), may hold values from -1.5 to 1.5
- train_mixed: bfloat16 [8192, 8192], P('model', 'rows'), may hold values from -0.0625 to 0.0625
- low_mixed: bfloat16 [8192, 16], P('model'), may hold values from -0.0625 to 0.0625
- high_mixed: bfloat16 [16, 8192], P(None, 'rows'), may hold values from -1.5 to 1.5
- norm_train: float32 [8192], P(('rows', 'model')), may hold values from 0.25 to 1.75
- norm_step: float32 [8192], P(('rows', 'model')), may hold values from -0.3 to 0.3
Outputs:
- serving_query: bfloat16 [8192, 8192], P('model')
- serving_key: bfloat16 [1024, 8192], P('model')
- serving_value: bfloat16 [1024, 8192], P('model')
- serving_mixed: bfloat16 [8192, 8192], P(None, 'model')
- serve_norm: bfloat16 [8192], replicated
The draws below stay inside these ranges and needn't reach their ends.
All inputs are finite; a program needn't handle non-finite values.
Results may differ from the reference program's by a relative error of at most 0.001.
Values may be sent and summed in bfloat16 or wider, within the bound.
A program may use at most 128 MiB of HBM per device.

```python
import jax
import jax.numpy as jnp

D_MODEL = 8192
Q_DIM = 8192
KV_DIM = 1024
RANK = 16


def level_of(key, dims, pieces, least, top_value):
    gain, own = 1.0, jax.random.fold_in(key, 6)
    for position, parts in pieces:
        heights = jnp.exp(jax.random.uniform(jax.random.fold_in(own, position), (parts,), jnp.float32, least / len(pieces), top_value / len(pieces)))
        gain = gain * jnp.repeat(heights, dims[position] // parts).reshape([-1 if axis == position else 1 for axis in range(len(dims))])
    return gain


def normal_values(stream_key, shape, width, limit, pieces=(), dtype=jnp.bfloat16):
    level = level_of(stream_key, shape, pieces, -0.22, 0.18) if pieces else 1.0
    values = jax.random.normal(stream_key, shape, jnp.float32) * width * level
    return jnp.minimum(jnp.maximum(values, -limit), limit).astype(dtype)


def setup_inputs(seed: int = 0) -> dict:
    key_of = jax.random.split(jax.random.key(seed), 15)
    train_query = normal_values(key_of[0], (D_MODEL, Q_DIM), D_MODEL ** -0.5, 0.0625, ((0, 4), (1, 8)))
    low_query = normal_values(key_of[1], (D_MODEL, RANK), D_MODEL ** -0.5, 0.0625, ((0, 4),))
    high_query = normal_values(key_of[2], (RANK, Q_DIM), RANK ** -0.5, 1.5, ((1, 8),))
    train_key = normal_values(key_of[3], (D_MODEL, KV_DIM), D_MODEL ** -0.5, 0.0625, ((0, 4), (1, 8)))
    low_key = normal_values(key_of[4], (D_MODEL, RANK), D_MODEL ** -0.5, 0.0625, ((0, 4),))
    high_key = normal_values(key_of[5], (RANK, KV_DIM), RANK ** -0.5, 1.5, ((1, 8),))
    train_value = normal_values(key_of[6], (D_MODEL, KV_DIM), D_MODEL ** -0.5, 0.0625, ((0, 4), (1, 8)))
    low_value = normal_values(key_of[7], (D_MODEL, RANK), D_MODEL ** -0.5, 0.0625, ((0, 4),))
    high_value = normal_values(key_of[8], (RANK, KV_DIM), RANK ** -0.5, 1.5, ((1, 8),))
    train_mixed = normal_values(key_of[9], (Q_DIM, D_MODEL), Q_DIM ** -0.5, 0.0625, ((0, 8), (1, 4)))
    low_mixed = normal_values(key_of[10], (Q_DIM, RANK), Q_DIM ** -0.5, 0.0625, ((0, 8),))
    high_mixed = normal_values(key_of[11], (RANK, D_MODEL), RANK ** -0.5, 1.5, ((1, 4),))
    norm_train = jnp.clip(1.0 + 0.15 * jax.random.normal(key_of[12], (D_MODEL,), jnp.float32), 0.25, 1.75)
    norm_step = jnp.clip(jax.random.uniform(key_of[13], (D_MODEL,), jnp.float32, -0.3, 0.3) * level_of(key_of[13], (D_MODEL,), ((0, 32),), -0.4, 0.0), -0.3, 0.3)
    return dict(train_query=train_query, low_query=low_query, high_query=high_query, train_key=train_key, low_key=low_key, high_key=high_key, train_value=train_value, low_value=low_value, high_value=high_value, train_mixed=train_mixed, low_mixed=low_mixed, high_mixed=high_mixed, norm_train=norm_train, norm_step=norm_step)


mix_rate = 0.5


def reference(train_query, low_query, high_query, train_key, low_key, high_key, train_value, low_value, high_value, train_mixed, low_mixed, high_mixed, norm_train, norm_step):
    whole_query = train_query.astype(jnp.float32) + mix_rate * jnp.dot(low_query, high_query, preferred_element_type=jnp.float32)
    whole_key = train_key.astype(jnp.float32) + mix_rate * jnp.dot(low_key, high_key, preferred_element_type=jnp.float32)
    whole_value = train_value.astype(jnp.float32) + mix_rate * jnp.dot(low_value, high_value, preferred_element_type=jnp.float32)
    whole_mixed = train_mixed.astype(jnp.float32) + mix_rate * jnp.dot(low_mixed, high_mixed, preferred_element_type=jnp.float32)
    serving_query = whole_query.T.astype(jnp.bfloat16)
    serving_key = whole_key.T.astype(jnp.bfloat16)
    serving_value = whole_value.T.astype(jnp.bfloat16)
    serving_mixed = whole_mixed.T.astype(jnp.bfloat16)
    serve_norm = (norm_train + norm_step).astype(jnp.bfloat16)
    return serving_query, serving_key, serving_value, serving_mixed, serve_norm
```

```python
import jax
import jax.numpy as jnp
from jax import lax
from jax.experimental import pallas as pl
from jax.experimental.pallas import tpu as pltpu
from jax.sharding import PartitionSpec as P


mix_rate = 0.5


def merge_kernel(train_ref, low_ref, high_ref, out_ref):
    change = lax.dot_general(
        high_ref[...], low_ref[...], (((0,), (0,)), ((), ())), preferred_element_type=jnp.float32
    )
    whole = train_ref[...].T.astype(jnp.float32) + mix_rate * change
    out_ref[...] = whole.astype(out_ref.dtype)


def merged(train, low, high, part, parts):
    depth, width = train.shape
    rank = low.shape[1]
    tile = min(256 if depth <= 1024 else 128, width // parts)
    tiles = width // parts // tile
    return pl.pallas_call(
        merge_kernel,
        grid=(tiles,),
        in_specs=[
            pl.BlockSpec((depth, tile), lambda i: (0, part * tiles + i)),
            pl.BlockSpec((rank, depth), lambda i: (0, 0)),
            pl.BlockSpec((rank, tile), lambda i: (0, part * tiles + i)),
        ],
        out_specs=pl.BlockSpec((tile, depth), lambda i: (i, 0)),
        out_shape=jax.ShapeDtypeStruct((width // parts, depth), train.dtype),
        cost_estimate=pl.CostEstimate(
            flops=2 * rank * depth * width // parts,
            bytes_accessed=4 * depth * width // parts,
            transcendentals=0,
        ),
        name="merge",
    )(train, low.T, high)


def place_kernel(owner_ref, *refs):
    refs[-1][...] = refs[-2][...]


def placed(whole, piece, owner, shape, axis, part, parts):
    rows, width = piece.shape
    tile = min(rows, 256)
    tiles = rows // tile
    if axis == 1:
        spot = lambda i, owner: (part * tiles + i, owner[0])
    else:
        spot = lambda i, owner: ((owner[0] * parts + part) * tiles + i, 0)
    before = [] if whole is None else [whole]
    return pl.pallas_call(
        place_kernel,
        grid_spec=pltpu.PrefetchScalarGridSpec(
            num_scalar_prefetch=1,
            grid=(tiles,),
            in_specs=[pl.BlockSpec(memory_space=pl.ANY)] * len(before)
            + [pl.BlockSpec((tile, width), lambda i, owner: (i, 0))],
            out_specs=pl.BlockSpec((tile, width), spot),
        ),
        out_shape=jax.ShapeDtypeStruct(shape, piece.dtype),
        input_output_aliases={1: 0} if before else {},
        cost_estimate=pl.CostEstimate(
            flops=0, bytes_accessed=4 * rows * width, transcendentals=0
        ),
        name="place",
    )(owner, *before, piece)


def after(value, earlier):
    return lax.optimization_barrier((value, earlier))


def order(step, count):
    return list(range(count)) if step == 1 else list(range(2, count)) + [0, 1]


def body(
    train_query,
    low_query,
    high_query,
    train_key,
    low_key,
    high_key,
    train_value,
    low_value,
    high_value,
    train_mixed,
    low_mixed,
    high_mixed,
    norm_train,
    norm_step,
):
    n = lax.axis_size("rows")
    me = lax.axis_index("rows")
    ring = [(i, (i + 1) % n) for i in range(n)]
    owners = [jnp.reshape(lax.rem(me - step + n, n), (1,)).astype(jnp.int32) for step in range(n)]

    weights = {
        "key": (train_key, low_key, high_key, 1),
        "value": (train_value, low_value, high_value, 1),
        "query": (train_query, low_query, high_query, 1),
        "mixed": (train_mixed, low_mixed, high_mixed, 0),
    }
    plan = [
        ("key", 0, 1),
        ("value", 0, 1),
        ("query", 0, 2),
        ("query", 1, 2),
        ("mixed", 0, 2),
        ("mixed", 1, 2),
    ]
    shapes, outs = {}, {}
    for name, (train, _, _, axis) in weights.items():
        shape = [train.shape[1], train.shape[0]]
        shape[axis] *= n
        shapes[name] = tuple(shape)
        outs[name] = None

    def place(number, piece, step):
        name, part, parts = plan[number]
        outs[name] = placed(
            outs[name], piece, owners[step], shapes[name], weights[name][3], part, parts
        )
        return name

    gain = (norm_train + norm_step).astype(jnp.bfloat16)
    gain = lax.all_gather(gain, "model", axis=0, tiled=True)

    own = []
    for name, part, parts in plan:
        train, low, high, _ = weights[name]
        if own:
            high, own[-1] = after(high, own[-1])
        own.append(merged(train, low, high, part, parts))
    moving = list(own)
    serve_norm = lax.dynamic_update_slice_in_dim(
        jnp.zeros((n, gain.shape[0]), gain.dtype), gain[None], me, 0
    )
    last = None
    for step in range(1, n):
        turn = order(step, len(plan))
        arrived = {}
        for number in turn:
            piece = moving[number]
            if last is not None:
                piece, outs[last] = after(piece, outs[last])
            arrived[number] = lax.ppermute(piece, "rows", ring)
            if step > 1:
                last = place(number, piece, step - 1)
        if step == 1:
            for number in turn:
                last = place(number, own[number], 0)
        gain = lax.ppermute(gain, "rows", ring)
        serve_norm = lax.dynamic_update_slice_in_dim(
            serve_norm, gain[None], owners[step][0], 0
        )
        moving = [arrived[number] for number in range(len(plan))]
    for number in order(n - 1, len(plan)):
        place(number, moving[number], n - 1)
    serve_norm = jnp.reshape(serve_norm, (-1,))
    return (outs["query"], outs["key"], outs["value"], outs["mixed"], serve_norm)


def solution(mesh):
    return jax.shard_map(
        body,
        mesh=mesh,
        in_specs=(
            P("rows", "model"),
            P("rows", None),
            P(None, "model"),
            P("rows", "model"),
            P("rows", None),
            P(None, "model"),
            P("rows", "model"),
            P("rows", None),
            P(None, "model"),
            P("model", "rows"),
            P("model", None),
            P(None, "rows"),
            P(("rows", "model")),
            P(("rows", "model")),
        ),
        out_specs=(P("model", None), P("model", None), P("model", None), P(None, "model"), P()),
        check_vma=False,
    )
```

```python
import jax
import jax.numpy as jnp
from jax import lax
from jax.experimental import pallas as pl
from jax.experimental.pallas import tpu as pltpu
from jax.sharding import PartitionSpec as P


mix_rate = 0.5


def merge_kernel(train_ref, low_ref, high_ref, out_ref):
    change = lax.dot_general(
        high_ref[...], low_ref[...], (((0,), (0,)), ((), ())), preferred_element_type=jnp.float32
    )
    whole = train_ref[...].T.astype(jnp.float32) + mix_rate * change
    out_ref[...] = whole.astype(out_ref.dtype)


def merged(train, low, high, cut, part, parts):
    depth, width = train.shape
    rank = low.shape[0]
    if cut == 0:
        width = width // parts
        tile = min(256 if depth <= 1024 else 128, width)
        tiles, first, across = width // tile, part * (width // tile), 0
    else:
        depth = depth // parts
        tile = width
        tiles, first, across = 1, 0, part
    return pl.pallas_call(
        merge_kernel,
        grid=(tiles,),
        in_specs=[
            pl.BlockSpec((depth, tile), lambda i: (across, first + i)),
            pl.BlockSpec((rank, depth), lambda i: (0, across)),
            pl.BlockSpec((rank, tile), lambda i: (0, first + i)),
        ],
        out_specs=pl.BlockSpec((tile, depth), lambda i: (i, 0)),
        out_shape=jax.ShapeDtypeStruct((width, depth), train.dtype),
        cost_estimate=pl.CostEstimate(
            flops=2 * rank * depth * width,
            bytes_accessed=4 * depth * width,
            transcendentals=0,
        ),
        name="merge",
    )(train, low, high)


def place_kernel(owner_ref, *refs):
    refs[-1][...] = refs[-2][...]


def placed(whole, piece, owner, shape, axis, cut, part, parts):
    rows, width = piece.shape
    tile = min(rows, 256)
    tiles = rows // tile
    if axis == 0:
        spot = lambda i, owner: ((owner[0] * parts + part) * tiles + i, 0)
    elif cut == 0:
        spot = lambda i, owner: (part * tiles + i, owner[0])
    else:
        spot = lambda i, owner: (i, owner[0] * parts + part)
    before = [] if whole is None else [whole]
    return pl.pallas_call(
        place_kernel,
        grid_spec=pltpu.PrefetchScalarGridSpec(
            num_scalar_prefetch=1,
            grid=(tiles,),
            in_specs=[pl.BlockSpec(memory_space=pl.ANY)] * len(before)
            + [pl.BlockSpec((tile, width), lambda i, owner: (i, 0))],
            out_specs=pl.BlockSpec((tile, width), spot),
        ),
        out_shape=jax.ShapeDtypeStruct(shape, piece.dtype),
        input_output_aliases={1: 0} if before else {},
        cost_estimate=pl.CostEstimate(
            flops=0, bytes_accessed=4 * rows * width, transcendentals=0
        ),
        name="place",
    )(owner, *before, piece)


def after(value, earlier):
    return lax.optimization_barrier((value, earlier))


plan = [
    ("key", 0, 0, 1),
    ("value", 0, 0, 1),
    ("query", 0, 0, 2),
    ("query", 0, 1, 2),
    ("mixed", 0, 0, 2),
    ("mixed", 0, 1, 2),
]
small = 2


def order(step):
    count = len(plan)
    return list(range(count)) if step == 1 else list(range(small, count)) + list(range(small))


def body(
    train_query,
    low_query,
    high_query,
    train_key,
    low_key,
    high_key,
    train_value,
    low_value,
    high_value,
    train_mixed,
    low_mixed,
    high_mixed,
    norm_train,
    norm_step,
):
    n = lax.axis_size("rows")
    me = lax.axis_index("rows")
    ring = [(i, (i + 1) % n) for i in range(n)]
    owners = [jnp.reshape(lax.rem(me - step + n, n), (1,)).astype(jnp.int32) for step in range(n)]

    weights = {
        "key": (train_key, low_key, high_key, 1),
        "value": (train_value, low_value, high_value, 1),
        "query": (train_query, low_query, high_query, 1),
        "mixed": (train_mixed, low_mixed, high_mixed, 0),
    }
    shapes, outs = {}, {}
    for name, (train, _, _, axis) in weights.items():
        shape = [train.shape[1], train.shape[0]]
        shape[axis] *= n
        shapes[name] = tuple(shape)
        outs[name] = None

    def place(number, piece, step):
        name, cut, part, parts = plan[number]
        axis = weights[name][3]
        outs[name] = placed(
            outs[name], piece, owners[step], shapes[name], axis, cut, part, parts
        )
        return name

    gain = (norm_train + norm_step).astype(jnp.bfloat16)
    gain = lax.all_gather(gain, "model", axis=0, tiled=True)

    own, previous = {}, None
    for number in list(range(1, len(plan))) + [0]:
        name, cut, part, parts = plan[number]
        train, low, high, _ = weights[name]
        if previous is not None:
            high, own[previous] = after(high, own[previous])
        own[number] = merged(train, low.T, high, cut, part, parts)
        previous = number
    moving = [own[number] for number in range(len(plan))]
    moving[0] = train_key
    share = low_key.shape[0] // lax.axis_size("model")
    low_share = lax.dynamic_slice_in_dim(
        low_key.T, lax.axis_index("model") * share, share, 1
    )
    low_share = lax.ppermute(low_share, "rows", ring)
    serve_norm = lax.dynamic_update_slice_in_dim(
        jnp.zeros((n, gain.shape[0]), gain.dtype), gain[None], me, 0
    )
    last = None
    for step in range(1, n):
        turn = order(step)
        arrived = {}
        for number in turn:
            piece = moving[number]
            if last is not None:
                piece, outs[last] = after(piece, outs[last])
            arrived[number] = lax.ppermute(piece, "rows", ring)
            if step > 1:
                last = place(number, piece, step - 1)
        if step == 1:
            low_moved = lax.all_gather(low_share, "model", axis=1, tiled=True)
            arrived[0] = merged(arrived[0], low_moved, high_key, *plan[0][1:])
            for number in turn:
                last = place(number, own[number], 0)
        gain = lax.ppermute(gain, "rows", ring)
        serve_norm = lax.dynamic_update_slice_in_dim(
            serve_norm, gain[None], owners[step][0], 0
        )
        moving = [arrived[number] for number in range(len(plan))]
    for number in order(n - 1):
        place(number, moving[number], n - 1)
    serve_norm = jnp.reshape(serve_norm, (-1,))
    return (outs["query"], outs["key"], outs["value"], outs["mixed"], serve_norm)


def solution(mesh):
    return jax.shard_map(
        body,
        mesh=mesh,
        in_specs=(
            P("rows", "model"),
            P("rows", None),
            P(None, "model"),
            P("rows", "model"),
            P("rows", None),
            P(None, "model"),
            P("rows", "model"),
            P("rows", None),
            P(None, "model"),
            P("model", "rows"),
            P("model", None),
            P(None, "rows"),
            P(("rows", "model")),
            P(("rows", "model")),
        ),
        out_specs=(P("model", None), P("model", None), P("model", None), P(None, "model"), P()),
        check_vma=False,
    )
```
